32 devices in a mesh: row: 8 (over z, x), col: 4 (over y, core).
Axes of the slice: x: 2, y: 2, z: 4, core: 2. Of those that a mesh axis runs over, the one named last changes fastest.
Arguments:
- amplitudes: float32 [200, 10, 10, 1024], P('row', None, None, 'col'), may hold values from -6 to 6
- old_blocks: int32 [8, 25], replicated, may hold values from 0 to 135, as said below
- old_counts: int32 [8], replicated, may hold values from 1 to 25, as said below
- new_phase: int32 [1], replicated, may hold values from 0 to 7
- fock: float32 [160, 160], P('row'), may hold values from -0.5 to 0.5
Outputs:
- contracted: float32 [16, 10, 160, 1024], P('row', None, None, 'col')
The draws below stay inside these ranges and needn't reach their ends.
Inputs may be any that keep to these rules, and one draw needn't show every extreme that they name: `old_blocks`: over the live slots of all row devices every tile pair id 0 to 135 stands exactly once; ids in slots that are not live are arbitrary. For every residue r mod 8, at most 8 live blocks of one row device hold a tile whose index is r mod 8, and some device reaches 8 for some r. `old_counts`: the counts sum to 136; some device has exactly 25.
All inputs are finite; a program needn't handle non-finite values.
Results may differ from the reference program's by a relative error of at most 0.00007.
Values sent between devices are 32-bit elements; how exact they have to be, the bound alone decides.
No kernel may reach another device: no remote copies, remote signals or barrier semaphores. Data moves between devices by JAX's collectives and lax.ppermute only.
A program may use at most 128 MiB of HBM per device.

```python
import jax
import jax.numpy as jnp
import numpy as np
from jax import lax

V = 160
NT = 16
BT = 10
OPAIRS = 1024
SLOTS = 25
N_ROW = 8


def tile_lists():
    count = NT * (NT + 1) // 2
    first_tile = np.zeros((count,), np.int32)
    second_tile = np.zeros((count,), np.int32)
    for low in range(NT):
        for high in range(low, NT):
            ident = low * NT - low * (low - 1) // 2 + (high - low)
            first_tile[ident] = low
            second_tile[ident] = high
    return (first_tile, second_tile)


def layout_tables(key):
    inner = jax.random.fold_in(key, 7)
    key_full, key_extra, key_res, key_odd, key_rest, key_noise, key_junk = jax.random.split(inner, 7)
    nblocks = NT * (NT + 1) // 2
    first_np, second_np = tile_lists()
    first_tile = jnp.asarray(first_np)
    second_tile = jnp.asarray(second_np)
    residue = jax.random.randint(key_res, (), 0, N_ROW)
    owned = ((first_tile % N_ROW == residue) | (second_tile % N_ROW == residue)).astype(jnp.int32)
    klass = (first_tile + second_tile) % NT
    odd_order = 2 * jax.random.permutation(key_odd, NT // 2).astype(jnp.int32) + 1
    evens = 2 * jnp.arange(NT // 2, dtype=jnp.int32)
    leftover = jax.random.permutation(key_rest, jnp.concatenate([odd_order[4:], evens])).astype(jnp.int32)
    order = jnp.concatenate([odd_order[:4], leftover]).astype(jnp.int32)
    rank = jnp.zeros((NT,), jnp.int32).at[order].set(jnp.arange(NT, dtype=jnp.int32))
    block_rank = rank[klass]
    noise = jax.random.permutation(key_noise, nblocks).astype(jnp.int32)
    group = jnp.where((block_rank == 0) & (owned == 1), 0, jnp.where(block_rank == 0, 100, block_rank))
    sort_key = group * 1000 + (1 - owned) * 200 + noise
    sequence = jnp.argsort(sort_key, stable=True).astype(jnp.int32)
    full = jax.random.randint(key_full, (), 0, N_ROW)
    rest = nblocks - SLOTS
    base = rest // (N_ROW - 1)
    extra = rest - base * (N_ROW - 1)
    shuffle = jax.random.permutation(key_extra, N_ROW - 1)
    others = base + (shuffle < extra).astype(jnp.int32)
    pos_counts = jnp.concatenate([jnp.full((1,), SLOTS, jnp.int32), others.astype(jnp.int32)])
    pos_starts = jnp.cumsum(pos_counts) - pos_counts
    device = jnp.arange(N_ROW, dtype=jnp.int32)
    place = (device - full) % N_ROW
    counts = pos_counts[place].astype(jnp.int32)
    starts = pos_starts[place]
    slot = jnp.arange(SLOTS, dtype=jnp.int32)[None, :]
    where_at = jnp.clip(starts[:, None] + slot, 0, nblocks - 1)
    junk = jax.random.randint(key_junk, (N_ROW, SLOTS), 0, nblocks)
    blocks = jnp.where(slot < counts[:, None], sequence[where_at], junk).astype(jnp.int32)
    return (blocks, counts)


def draw_old_blocks(key, part):
    return layout_tables(key)[0]


def draw_old_counts(key, part):
    return layout_tables(key)[1]


def block_levels(stream_key, extent, cuts, smallest, high):
    def one(dim, parts):
        draws = jax.random.uniform(jax.random.fold_in(jax.random.fold_in(stream_key, 6), dim), (parts,), jnp.float32, smallest / len(cuts), high / len(cuts))
        return jnp.repeat(jnp.exp(draws), extent[dim] // parts).reshape((-1,) + (1,) * (len(extent) - dim - 1))

    factor_of = one(*cuts[0])
    for cut in cuts[1:]:
        factor_of = factor_of * one(*cut)
    return factor_of


def normal_values(rng, shape, deviation, most, cuts=(), kind=jnp.bfloat16):
    gain = block_levels(rng, shape, cuts, -0.22, 0.18) if cuts else 1.0
    drawn = jax.random.normal(rng, shape, jnp.float32) * deviation * gain
    return jnp.minimum(jnp.maximum(drawn, -most), most).astype(kind)


def setup_inputs(seed: int = 0) -> dict:
    seeds = jax.random.split(jax.random.key(seed), 6)
    return {
        "amplitudes": normal_values(seeds[0], (N_ROW * SLOTS, BT, BT, OPAIRS), 1.0, 6.0, ((0, 8), (3, 4)), jnp.float32),
        "old_blocks": draw_old_blocks(jax.random.fold_in(seeds[5], 71), 0),
        "old_counts": draw_old_counts(jax.random.fold_in(seeds[5], 71), 0),
        "new_phase": jax.random.randint(seeds[3], (1,), 0, N_ROW).astype(jnp.int32),
        "fock": normal_values(seeds[4], (V, V), V ** -0.5, 0.5, ((0, 8),), jnp.float32),
    }


def pair_table():
    table = np.zeros((NT, NT), np.int32)
    for first in range(NT):
        for second in range(NT):
            low = min(first, second)
            high = max(first, second)
            table[first, second] = low * NT - low * (low - 1) // 2 + (high - low)
    return table


def reference(amplitudes, old_blocks, old_counts, new_phase, fock):
    nblocks = NT * (NT + 1) // 2
    live = jnp.arange(SLOTS, dtype=jnp.int32)[None, :] < old_counts[:, None]
    target = jnp.where(live, old_blocks, nblocks).reshape(-1).astype(jnp.int32)
    blocks = jnp.zeros((nblocks, BT, BT, amplitudes.shape[3]), jnp.float32)
    blocks = blocks.at[target].set(amplitudes, mode="drop")
    table = jnp.asarray(pair_table())
    upper = blocks[table.reshape(-1)].reshape(NT, NT, BT, BT, -1)
    upper = jnp.transpose(upper, (0, 2, 1, 3, 4)).reshape(V, V, -1)
    index = jnp.arange(V, dtype=jnp.int32)
    lower_mask = (index[:, None] < index[None, :])[:, :, None]
    upper_mask = (index[:, None] > index[None, :])[:, :, None]
    dense = jnp.where(lower_mask, upper, jnp.where(upper_mask, -jnp.swapaxes(upper, 0, 1), 0.0))
    half = jnp.einsum("ac,cbj->baj", fock, dense, precision=lax.Precision.HIGHEST)
    per_dev = NT // N_ROW
    position = jnp.arange(NT, dtype=jnp.int32)
    owner = position // per_dev
    within = position % per_dev
    tiles = (owner - new_phase[0]) % N_ROW + within * N_ROW
    return half.reshape(NT, BT, V, -1)[tiles.astype(jnp.int32)]
```

```python
import functools

import jax
import jax.numpy as jnp
from jax import lax
from jax.experimental import pallas as pl
from jax.experimental.pallas import tpu as pltpu
from jax.sharding import PartitionSpec as P


NT = 16
LANES = 128
VMEM_LIMIT = 60 * 2**20


class Plan:
    def __init__(self, nrows, slots):
        self.nrows = nrows
        self.half = nrows // 2
        self.per = NT // nrows
        self.cap = self.per * ((slots - 2) // 8 + 2)
        self.fwd = self.per * self.per
        self.n_send = nrows * self.cap
        self.n_fwd = (self.half - 1) * self.fwd
        self.n_loc = self.per * NT
        self.at_fwd = self.n_send
        self.at_loc = self.n_send + self.n_fwd
        self.at_level = self.at_loc + self.n_loc
        cap = self.cap
        wide = -(-5 * cap // 8), -(-6 * cap // 8), cap
        early = -(-cap // 2), -(-cap // 2), cap
        self.levels = tuple(zip(wide, early))


def route_kernel(plan, slots, ids_ref, counts_ref, phase_ref, out_ref):
    nrows, half, per, cap = plan.nrows, plan.half, plan.per, plan.cap
    me = lax.axis_index("row")
    phase = phase_ref[0]
    ids = ids_ref[...]
    first = jnp.zeros_like(ids)
    for t in range(1, NT):
        first = first + (ids >= t * NT - t * (t - 1) // 2).astype(jnp.int32)
    second = ids - (first * NT - lax.shift_right_logical(first * (first - 1), 1)) + first
    src = lax.broadcasted_iota(jnp.int32, ids.shape, 1)
    slot = lax.broadcasted_iota(jnp.int32, ids.shape, 0)
    live = slot < counts_ref[...]
    low = (first + phase) & (nrows - 1)
    high = (second + phase) & (nrows - 1)
    shift = nrows.bit_length() - 1
    w_low = lax.shift_right_logical(first, shift)
    w_high = lax.shift_right_logical(second, shift)
    pair_part = jnp.where(low < high, w_low * per + w_high, w_high * per + w_low)
    far_low = ((low ^ src) & half) != 0
    far_high = ((high ^ src) & half) != 0
    same = low == high
    one = jnp.int32(1)
    zero = jnp.int32(0)

    def flag(x):
        return jnp.where(x, one, zero)

    in_low = flag(live & ~far_low)
    in_high = flag(live & ~far_high & ~same)
    x_low = flag(live & far_low)
    x_high = flag(live & far_high & ~same)
    both = x_low * x_high
    single = x_low + x_high - 2 * both
    goal = jnp.where(x_low == 1, low, high)
    dest = lax.broadcasted_iota(jnp.int32, (nrows, nrows), 0)

    def row(x, s):
        return x[s : s + 1, :]

    def hit(x, on, s):
        return jnp.where((dest == row(x, s)) & (row(on, s) == 1), 1.0, 0.0)

    def at(mask, run):
        return jnp.sum(mask * run, axis=0, keepdims=True)

    count = jnp.zeros((nrows, nrows), jnp.float32)
    singles = []
    for s in range(slots):
        mask = hit(goal, single, s)
        singles.append(mask)
        count = count + mask
    early = jnp.zeros((nrows, nrows), jnp.float32)
    land_rows, pos_rows = [], []
    for s in range(slots):
        m_low = hit(low, both, s)
        m_high = hit(high, both, s)
        take = at(m_low, count) <= at(m_high, count)
        mask = jnp.where(take, m_low, m_high)
        pos_rows.append(at(mask, early))
        land_rows.append(jnp.where(take, row(low, s), row(high, s)))
        early = early + mask
        count = count + mask
    run = early
    for s in range(slots):
        pos_rows[s] = pos_rows[s] + at(singles[s], run)
        run = run + singles[s]
    run_in = jnp.zeros((nrows, nrows), jnp.float32)
    low_rows, high_rows = [], []
    for s in range(slots):
        m_low = hit(low, in_low, s)
        m_high = hit(high, in_high, s)
        low_rows.append(at(m_low, run_in))
        high_rows.append(at(m_high, run_in))
        run_in = run_in + m_low + m_high

    def top(x):
        return jnp.max(jnp.max(x, axis=0, keepdims=True), axis=1, keepdims=True)

    most, most_early = top(count), top(early)
    level = jnp.full((1, 1), float(len(plan.levels) - 1), jnp.float32)
    for i in range(len(plan.levels) - 2, -1, -1):
        wide, soon = plan.levels[i]
        level = jnp.where((most <= wide) & (most_early <= soon), float(i), level)

    lane = lax.broadcasted_iota(jnp.int32, (1, nrows), 1)
    e_send = lax.broadcasted_iota(jnp.int32, (plan.n_send, nrows), 0)
    e_fwd = lax.broadcasted_iota(jnp.int32, (plan.n_fwd, nrows), 0)
    e_loc = lax.broadcasted_iota(jnp.int32, (plan.n_loc, nrows), 0)
    t_send = jnp.zeros((plan.n_send, nrows), jnp.int32)
    t_fwd = jnp.zeros((plan.n_fwd, nrows), jnp.int32)
    t_loc = jnp.zeros((plan.n_loc, nrows), jnp.int32)
    mine = lane == me

    def put(table, index, where_, value, on):
        return table + jnp.where(index == jnp.where(on, where_, -1), value, 0)

    for s in range(slots):
        lo, hi = row(low, s), row(high, s)
        il, ih = row(in_low, s) == 1, row(in_high, s) == 1
        bo, si = row(both, s) == 1, row(single, s) == 1
        p_low = low_rows[s].astype(jnp.int32)
        p_high = high_rows[s].astype(jnp.int32)
        p_far = pos_rows[s].astype(jnp.int32)
        land = jnp.where(bo, land_rows[s], row(goal, s))
        other = lo + hi - land
        k_land = (land ^ lane) * cap + p_far
        value = jnp.full((1, nrows), s, jnp.int32)
        t_send = put(t_send, e_send, (lo ^ lane) * cap + p_low, value, il & mine)
        t_send = put(t_send, e_send, (hi ^ lane) * cap + p_high, value, ih & mine)
        t_send = put(t_send, e_send, k_land, value, (bo | si) & mine)
        part = row(pair_part, s)
        t_fwd = put(t_fwd, e_fwd, ((land ^ other) - 1) * plan.fwd + part, k_land, bo & (land == me))
        near = ((lane ^ me) & half) == 0
        lo_me = lo == me
        hi_me = hi == me
        ok = row(flag(live), s) == 1
        code_near = (lane ^ me) * cap + jnp.where(lo_me, p_low, p_high)
        code_fwd = plan.at_fwd + ((land ^ me) - 1) * plan.fwd + part
        code_far = jnp.where(bo & (land != me), code_fwd, k_land)
        code = jnp.where(near, code_near, code_far)
        a, b = row(first, s), row(second, s)
        t_loc = put(t_loc, e_loc, row(w_low, s) * NT + b, code, ok & lo_me)
        t_loc = put(t_loc, e_loc, row(w_high, s) * NT + a, code, ok & hi_me & (a != b))

    def column(table):
        return jnp.sum(table.astype(jnp.float32), axis=1, keepdims=True)

    wide_lane = out_ref.shape[1]

    def spread(table, start):
        col = column(table)
        shape = (col.shape[0], wide_lane)
        down = lax.broadcasted_iota(jnp.int32, shape, 0) + start
        across = lax.broadcasted_iota(jnp.int32, shape, 1)
        return jnp.sum(jnp.where(down == across, col, 0.0), axis=0, keepdims=True)

    line = spread(t_send, 0) + spread(t_fwd, plan.at_fwd) + spread(t_loc, plan.at_loc)
    across = lax.broadcasted_iota(jnp.int32, (1, wide_lane), 1)
    line = jnp.where(across == plan.at_level, level, line)
    out_ref[...] = line.astype(jnp.int32)


def route(plan, old_blocks, old_counts, new_phase):
    nrows, slots = old_blocks.shape
    wide = -(-(plan.at_level + 1) // LANES) * LANES
    return pl.pallas_call(
        functools.partial(route_kernel, plan, slots),
        out_shape=jax.ShapeDtypeStruct((1, wide), jnp.int32),
        in_specs=[
            pl.BlockSpec(memory_space=pltpu.VMEM),
            pl.BlockSpec(memory_space=pltpu.VMEM),
            pl.BlockSpec(memory_space=pltpu.SMEM),
        ],
        out_specs=pl.BlockSpec(memory_space=pltpu.VMEM),
        name="route",
    )(old_blocks.T, old_counts.reshape(1, nrows), new_phase)


def pack_kernel(streams, slots_pad, parts, table_ref, *refs):
    rows = refs[0].shape[0]
    flats = [ref.reshape(rows * slots_pad, LANES) for ref in refs[:parts]]
    f_refs, outs = refs[parts:-len(streams)], refs[-len(streams) :]
    for (base, count, carries), out in zip(streams, outs):

        def one(j, carry, base=base, out=out):
            slot = table_ref[0, base + j]
            for h, flat in enumerate(flats):
                for r in range(0, rows, 8):
                    n = min(8, rows - r)
                    piece = flat[pl.ds(r * slots_pad + slot, n, stride=slots_pad), :]
                    out[pl.ds(j * rows * parts + h * rows + r, n), :] = piece
            return carry

        lax.fori_loop(0, count, one, 0)
        if carries:
            (f_ref,) = f_refs
            mine, wide = f_ref.shape
            for h in range(wide // LANES):
                at = count * rows * parts + h * mine
                out[pl.ds(at, mine), :] = f_ref[:, h * LANES : (h + 1) * LANES]


def fock_rows(f_mine):
    return -(-f_mine.shape[0] * (f_mine.shape[1] // LANES) // 8) * 8


def pack(table, amp, f_mine, streams):
    rows, slots, occ = amp.shape
    parts = occ // LANES
    pad = -(-slots // 8) * 8
    extra = fock_rows(f_mine)
    shapes = [(n * rows * parts + (extra if c else 0), LANES) for _, n, c in streams]
    f_args = [f_mine] if any(c for _, _, c in streams) else []
    return pl.pallas_call(
        functools.partial(pack_kernel, streams, pad, parts),
        out_shape=[jax.ShapeDtypeStruct(shape, jnp.float32) for shape in shapes],
        in_specs=[
            pl.BlockSpec(memory_space=pltpu.SMEM),
            *[pl.BlockSpec((rows, pad, LANES), lambda i, h=h: (0, 0, h)) for h in range(parts)],
            *[pl.BlockSpec(x.shape, lambda i: (0, 0)) for x in f_args],
        ],
        out_specs=[pl.BlockSpec(shape, lambda i: (0, 0)) for shape in shapes],
        grid=(1,),
        compiler_params=pltpu.CompilerParams(vmem_limit_bytes=VMEM_LIMIT),
        name="pack",
    )(table, *[amp] * parts, *f_args)


def forward_kernel(plan, soon, size, table_ref, *refs):
    ins, outs = refs[: plan.half], refs[plan.half :]
    for k, out in enumerate(outs):

        def one(j, carry, k=k, out=out):
            code = table_ref[0, plan.at_fwd + k * plan.fwd + j]
            for f in range(plan.half):
                start = (plan.half + f) * plan.cap

                @pl.when((code >= start) & (code < start + soon))
                def _(f=f, start=start):
                    to, of = pl.multiple_of(j * size, 8), pl.multiple_of((code - start) * size, 8)
                    out[pl.ds(to, size), :] = ins[f][pl.ds(of, size), :]

            return carry

        lax.fori_loop(0, plan.fwd, one, 0)


def forward(plan, table, landed, soon, size):
    return pl.pallas_call(
        functools.partial(forward_kernel, plan, soon, size),
        out_shape=[jax.ShapeDtypeStruct((plan.fwd * size, LANES), jnp.float32)]
        * (plan.half - 1),
        in_specs=[pl.BlockSpec(memory_space=pltpu.SMEM)]
        + [pl.BlockSpec(memory_space=pltpu.VMEM)] * plan.half,
        out_specs=[pl.BlockSpec(memory_space=pltpu.VMEM)] * (plan.half - 1),
        compiler_params=pltpu.CompilerParams(vmem_limit_bytes=VMEM_LIMIT),
        name="forward",
    )(table, *landed)


def split(x):
    high = x.astype(jnp.bfloat16)
    return high, (x - high.astype(jnp.float32)).astype(jnp.bfloat16)


def contract_kernel(plan, tile, parts, pieces, f_piece, table_ref, phase_ref, *refs):
    n = len(pieces)
    ins, out_ref, blocks, dense, f_raw, f_hi, f_lo, sems = refs[:n], *refs[n:]
    step = pl.program_id(0)
    rows = tile * tile
    size = rows * parts
    me = lax.axis_index("row")
    mine, extra = f_piece

    @pl.when(step == 0)
    def _():
        copies = []
        for i, (ref, (start, count, sender)) in enumerate(zip(ins, pieces)):
            got = blocks.at[pl.ds(start * size, count * size)]
            copies.append(pltpu.make_async_copy(ref.at[pl.ds(0, count * size)], got, sems.at[0, i]))
            if sender is not None:
                got = f_raw.at[me ^ sender]
                part = ref.at[pl.ds(count * size, extra)]
                copies.append(pltpu.make_async_copy(part, got, sems.at[1, i]))
        for copy in copies:
            copy.start()
        for copy in copies:
            copy.wait()
        for device in range(plan.nrows):
            for h in range(f_hi.shape[1] // LANES):
                high, low = split(f_raw[device, h * mine : (h + 1) * mine, :])
                at = pl.ds(device * mine, mine), pl.ds(h * LANES, LANES)
                f_hi[at] = high
                f_lo[at] = low

    within = step // tile
    b = step - within * tile
    column = ((me - phase_ref[0]) & (plan.nrows - 1)) + within * plan.nrows
    b_global = column * tile + b
    sub = lax.broadcasted_iota(jnp.int32, (8, LANES), 0)
    for a in range(NT):
        code = table_ref[0, plan.at_loc + within * NT + a]
        for h in range(parts):
            base = code * size + h * rows
            for r in range(0, 16, 8):
                c_global = a * tile + r + sub
                left = blocks[pl.ds(base + b + r * tile, 8, stride=tile), :]
                right = blocks[pl.ds(base + b * tile + r, 8), :]
                value = jnp.where(
                    c_global < b_global, left, jnp.where(c_global > b_global, -right, 0.0)
                )
                if r + 8 > tile:
                    value = jnp.where(sub < tile - r, value, 0.0)
                dense[pl.ds(a * 16 + r, 8), pl.ds(h * LANES, LANES)] = value
    hi, lo = split(dense[...])
    dot = functools.partial(jnp.dot, preferred_element_type=jnp.float32)
    out_ref[0, 0] = dot(f_hi[...], hi) + (dot(f_lo[...], hi) + dot(f_hi[...], lo))


def contract(plan, table, new_phase, buffers, f_piece, tile, occ):
    parts = occ // LANES
    size = tile * tile * parts
    total = plan.n_send + plan.n_fwd
    width = plan.nrows * f_piece[0]
    pieces = tuple(buffer[:3] for buffer in buffers)
    return pl.pallas_call(
        functools.partial(contract_kernel, plan, tile, parts, pieces, f_piece),
        grid=(plan.per * tile,),
        out_shape=jax.ShapeDtypeStruct((plan.per, tile, width, occ), jnp.float32),
        in_specs=[pl.BlockSpec(memory_space=pltpu.SMEM)] * 2
        + [pl.BlockSpec(memory_space=pl.ANY)] * len(buffers),
        out_specs=pl.BlockSpec((1, 1, width, occ), lambda i: (i // tile, i % tile, 0, 0)),
        scratch_shapes=[
            pltpu.VMEM((total * size + 16 * tile, LANES), jnp.float32),
            pltpu.VMEM((NT * 16, occ), jnp.float32),
            pltpu.VMEM((plan.nrows, f_piece[1], LANES), jnp.float32),
            pltpu.VMEM((width, NT * 16), jnp.bfloat16),
            pltpu.VMEM((width, NT * 16), jnp.bfloat16),
            pltpu.SemaphoreType.DMA((2, len(buffers))),
        ],
        compiler_params=pltpu.CompilerParams(
            dimension_semantics=("arbitrary",), vmem_limit_bytes=VMEM_LIMIT
        ),
        name="contract",
    )(table, new_phase, *[buffer[3] for buffer in buffers])


def body(amplitudes, old_blocks, old_counts, new_phase, fock):
    nrows = lax.axis_size("row")
    slots, tile, _, occ = amplitudes.shape
    plan = Plan(nrows, slots)
    half, cap = plan.half, plan.cap
    size = tile * tile * occ // LANES

    def send(x, k):
        return lax.ppermute(x, "row", [(i, i ^ k) for i in range(nrows)])

    table = route(plan, old_blocks, old_counts, new_phase)
    mine = fock.shape[0]
    f_mine = jnp.pad(fock.reshape(mine, NT, tile), ((0, 0), (0, 0), (0, 16 - tile)))
    f_mine = f_mine.reshape(mine, NT * 16)
    f_piece = mine, fock_rows(f_mine)
    amp = jnp.transpose(amplitudes, (1, 2, 0, 3)).reshape(tile * tile, slots, occ)

    def branch(wide, soon, table, amp, new_phase, f_mine):
        late = wide - soon
        far = range(half, nrows)
        head = pack(table, amp, f_mine, [(k * cap, soon, not late) for k in far])
        landed = [send(head[k - half], k) for k in far]
        rest = [(k * cap, cap, True) for k in range(half)]
        rest += [(k * cap + soon, late, True) for k in far] if late else []
        rest = pack(table, amp, f_mine, rest)
        near_in = [rest[0]] + [send(rest[k], k) for k in range(1, half)]
        late_in = [send(rest[k], k) for k in far] if late else []
        relay = forward(plan, table, landed, soon, size)
        relay_in = [send(x, k + 1) for k, x in enumerate(relay)]
        buffers = [(k * cap, cap, k, near_in[k]) for k in range(half)]
        buffers += [(k * cap, soon, None if late else k, landed[k - half]) for k in far]
        buffers += [(k * cap + soon, late, k, late_in[k - half]) for k in far if late]
        buffers += [(plan.at_fwd + k * plan.fwd, plan.fwd, None, x) for k, x in enumerate(relay_in)]
        return contract(plan, table, new_phase, buffers, f_piece, tile, occ)

    return lax.switch(
        table[0, plan.at_level],
        [functools.partial(branch, *level) for level in plan.levels],
        table,
        amp,
        new_phase,
        f_mine,
    )


def solution(mesh):
    return jax.shard_map(
        body,
        mesh=mesh,
        in_specs=(P("row", None, None, "col"), P(), P(), P(), P("row", None)),
        out_specs=P("row", None, None, "col"),
        check_vma=False,
    )
```

```python
import functools

import jax
import jax.numpy as jnp
from jax import lax
from jax.experimental import pallas as pl
from jax.experimental.pallas import tpu as pltpu
from jax.sharding import PartitionSpec as P


NT = 16
LANES = 128
VMEM_LIMIT = 60 * 2**20


class Plan:
    def __init__(self, nrows, slots):
        self.nrows = nrows
        self.half = nrows // 2
        self.quarter = nrows // 4
        self.per = NT // nrows
        self.cap = self.per * ((slots - 2) // 8 + 2)
        self.fwd = self.per * self.per
        self.n_send = nrows * self.cap
        self.n_fwd = (self.half - 1) * self.fwd
        self.n_loc = self.per * NT
        self.at_fwd = self.n_send
        self.at_loc = self.n_send + self.n_fwd
        self.at_level = self.at_loc + self.n_loc
        cap = self.cap
        part = [-(-i * cap // 8) for i in range(9)]
        levels = (
            (part[5], part[3], part[6]),
            (part[6], part[3], part[6]),
            (part[6], part[4], cap),
            (cap, cap, cap),
        )
        self.levels = tuple(dict.fromkeys(levels))


def route_kernel(plan, slots, ids_ref, counts_ref, phase_ref, out_ref):
    nrows, half, per, cap = plan.nrows, plan.half, plan.per, plan.cap
    me = lax.axis_index("row")
    phase = phase_ref[0]
    ids = ids_ref[...]
    first = jnp.zeros_like(ids)
    for t in range(1, NT):
        first = first + (ids >= t * NT - t * (t - 1) // 2).astype(jnp.int32)
    second = ids - (first * NT - lax.shift_right_logical(first * (first - 1), 1)) + first
    src = lax.broadcasted_iota(jnp.int32, ids.shape, 1)
    slot = lax.broadcasted_iota(jnp.int32, ids.shape, 0)
    live = slot < counts_ref[...]
    low = (first + phase) & (nrows - 1)
    high = (second + phase) & (nrows - 1)
    shift = nrows.bit_length() - 1
    w_low = lax.shift_right_logical(first, shift)
    w_high = lax.shift_right_logical(second, shift)
    pair_part = jnp.where(low < high, w_low * per + w_high, w_high * per + w_low)
    same = low == high
    one = jnp.int32(1)
    zero = jnp.int32(0)

    def flag(x):
        return jnp.where(x, one, zero)

    def group(owner):
        away = owner ^ src
        return jnp.where((away & half) != 0, 2, flag((away & plan.quarter) != 0))

    g_low, g_high = group(low), group(high)
    shared = flag(live & (g_low == g_high) & (g_low > 0) & ~same)
    on_low = flag(live) * (1 - shared)
    on_high = flag(live & ~same) * (1 - shared)
    dest = lax.broadcasted_iota(jnp.int32, (nrows, nrows), 0)
    away = dest ^ lax.broadcasted_iota(jnp.int32, (nrows, nrows), 1)
    is_far = (away & half) != 0
    is_next = ~is_far & ((away & plan.quarter) != 0)

    def row(x, s):
        return x[s : s + 1, :]

    def hit(x, on, s):
        return jnp.where((dest == row(x, s)) & (row(on, s) == 1), 1.0, 0.0)

    def at(mask, run):
        return jnp.sum(mask * run, axis=0, keepdims=True)

    count = jnp.zeros((nrows, nrows), jnp.float32)
    for s in range(slots):
        count = count + hit(low, on_low, s) + hit(high, on_high, s)
    early = jnp.zeros((nrows, nrows), jnp.float32)
    land_rows, pos_rows, low_rows, high_rows = [], [], [], []
    for s in range(slots):
        m_low = hit(low, shared, s)
        m_high = hit(high, shared, s)
        take = at(m_low, count) <= at(m_high, count)
        mask = jnp.where(take, m_low, m_high)
        pos_rows.append(at(mask, early))
        land_rows.append(jnp.where(take, row(low, s), row(high, s)))
        early = early + mask
        count = count + mask
    run = early
    for s in range(slots):
        m_low, m_high = hit(low, on_low, s), hit(high, on_high, s)
        low_rows.append(at(m_low, run))
        high_rows.append(at(m_high, run))
        run = run + m_low + m_high

    def top(x):
        return jnp.max(jnp.max(x, axis=0, keepdims=True), axis=1, keepdims=True)

    most = top(jnp.where(is_far, count, 0.0))
    most_early = top(jnp.where(is_far, early, 0.0))
    most_next = top(jnp.where(is_next, count, 0.0))
    level = jnp.full((1, 1), float(len(plan.levels) - 1), jnp.float32)
    for i in range(len(plan.levels) - 2, -1, -1):
        wide, soon, following = plan.levels[i]
        fits = (most <= wide) & (most_early <= soon) & (most_next <= following)
        level = jnp.where(fits, float(i), level)

    lane = lax.broadcasted_iota(jnp.int32, (1, nrows), 1)
    e_send = lax.broadcasted_iota(jnp.int32, (plan.n_send, nrows), 0)
    e_fwd = lax.broadcasted_iota(jnp.int32, (plan.n_fwd, nrows), 0)
    e_loc = lax.broadcasted_iota(jnp.int32, (plan.n_loc, nrows), 0)
    t_send = jnp.zeros((plan.n_send, nrows), jnp.int32)
    t_fwd = jnp.zeros((plan.n_fwd, nrows), jnp.int32)
    t_loc = jnp.zeros((plan.n_loc, nrows), jnp.int32)
    mine = lane == me

    def put(table, index, where_, value, on):
        return table + jnp.where(index == jnp.where(on, where_, -1), value, 0)

    for s in range(slots):
        lo, hi, land = row(low, s), row(high, s), land_rows[s]
        both = row(shared, s) == 1
        p_low = low_rows[s].astype(jnp.int32)
        p_high = high_rows[s].astype(jnp.int32)
        other = lo + hi - land
        k_low = (lo ^ lane) * cap + p_low
        k_high = (hi ^ lane) * cap + p_high
        k_land = (land ^ lane) * cap + pos_rows[s].astype(jnp.int32)
        value = jnp.full((1, nrows), s, jnp.int32)
        t_send = put(t_send, e_send, k_low, value, (row(on_low, s) == 1) & mine)
        t_send = put(t_send, e_send, k_high, value, (row(on_high, s) == 1) & mine)
        t_send = put(t_send, e_send, k_land, value, both & mine)
        part = row(pair_part, s)
        t_fwd = put(t_fwd, e_fwd, ((land ^ other) - 1) * plan.fwd + part, k_land, both & (land == me))
        lo_me, hi_me = lo == me, hi == me
        k_both = jnp.where(land == me, k_land, plan.at_fwd + ((land ^ me) - 1) * plan.fwd + part)
        code = jnp.where(both, k_both, jnp.where(lo_me, k_low, k_high))
        a, b = row(first, s), row(second, s)
        ok = row(flag(live), s) == 1
        t_loc = put(t_loc, e_loc, row(w_low, s) * NT + b, code, ok & lo_me)
        t_loc = put(t_loc, e_loc, row(w_high, s) * NT + a, code, ok & hi_me & (a != b))

    def column(table):
        return jnp.sum(table.astype(jnp.float32), axis=1, keepdims=True)

    wide_lane = out_ref.shape[1]

    def spread(table, start):
        col = column(table)
        shape = (col.shape[0], wide_lane)
        down = lax.broadcasted_iota(jnp.int32, shape, 0) + start
        across = lax.broadcasted_iota(jnp.int32, shape, 1)
        return jnp.sum(jnp.where(down == across, col, 0.0), axis=0, keepdims=True)

    line = spread(t_send, 0) + spread(t_fwd, plan.at_fwd) + spread(t_loc, plan.at_loc)
    across = lax.broadcasted_iota(jnp.int32, (1, wide_lane), 1)
    line = jnp.where(across == plan.at_level, level, line)
    out_ref[...] = line.astype(jnp.int32)


def route(plan, old_blocks, old_counts, new_phase):
    nrows, slots = old_blocks.shape
    wide = -(-(plan.at_level + 1) // LANES) * LANES
    return pl.pallas_call(
        functools.partial(route_kernel, plan, slots),
        out_shape=jax.ShapeDtypeStruct((1, wide), jnp.int32),
        in_specs=[
            pl.BlockSpec(memory_space=pltpu.VMEM),
            pl.BlockSpec(memory_space=pltpu.VMEM),
            pl.BlockSpec(memory_space=pltpu.SMEM),
        ],
        out_specs=pl.BlockSpec(memory_space=pltpu.VMEM),
        name="route",
    )(old_blocks.T, old_counts.reshape(1, nrows), new_phase)


def pack_kernel(streams, slots_pad, parts, table_ref, *refs):
    rows = refs[0].shape[0]
    flats = [ref.reshape(rows * slots_pad, LANES) for ref in refs[:parts]]
    f_refs, outs = refs[parts:-len(streams)], refs[-len(streams) :]
    for (base, count, carries), out in zip(streams, outs):

        def one(j, carry, base=base, out=out):
            slot = table_ref[0, base + j]
            for h, flat in enumerate(flats):
                for r in range(0, rows, 8):
                    n = min(8, rows - r)
                    piece = flat[pl.ds(r * slots_pad + slot, n, stride=slots_pad), :]
                    out[pl.ds(j * rows * parts + h * rows + r, n), :] = piece
            return carry

        lax.fori_loop(0, count, one, 0)
        if carries:
            write_fock(f_refs[0], out, count * rows * parts)


def fock_rows(f_mine):
    return -(-f_mine.shape[0] * (f_mine.shape[1] // LANES) // 8) * 8


def pack(table, amp, f_mine, streams):
    rows, slots, occ = amp.shape
    parts = occ // LANES
    pad = -(-slots // 8) * 8
    extra = fock_rows(f_mine)
    shapes = [(n * rows * parts + (extra if c else 0), LANES) for _, n, c in streams]
    f_args = [f_mine] if any(c for _, _, c in streams) else []
    return pl.pallas_call(
        functools.partial(pack_kernel, streams, pad, parts),
        out_shape=[jax.ShapeDtypeStruct(shape, jnp.float32) for shape in shapes],
        in_specs=[
            pl.BlockSpec(memory_space=pltpu.SMEM),
            *[pl.BlockSpec((rows, pad, LANES), lambda i, h=h: (0, 0, h)) for h in range(parts)],
            *[pl.BlockSpec(x.shape, lambda i: (0, 0)) for x in f_args],
        ],
        out_specs=[pl.BlockSpec(shape, lambda i: (0, 0)) for shape in shapes],
        grid=(1,),
        compiler_params=pltpu.CompilerParams(vmem_limit_bytes=VMEM_LIMIT),
        name="pack",
    )(table, *[amp] * parts, *f_args)


def forward_kernel(plan, size, ranges, table_ref, f_ref, *refs):
    ins, outs = refs[: len(ranges)], refs[len(ranges) :]
    for k, out in enumerate(outs):

        def one(j, carry, k=k, out=out):
            code = table_ref[0, plan.at_fwd + k * plan.fwd + j]
            for ref, (start, count) in zip(ins, ranges):

                @pl.when((code >= start) & (code < start + count))
                def _(ref=ref, start=start):
                    to, of = pl.multiple_of(j * size, 8), pl.multiple_of((code - start) * size, 8)
                    out[pl.ds(to, size), :] = ref[pl.ds(of, size), :]

            return carry

        lax.fori_loop(0, plan.fwd, one, 0)
        write_fock(f_ref, out, plan.fwd * size)


def write_fock(f_ref, out, start):
    mine, wide = f_ref.shape
    for h in range(wide // LANES):
        out[pl.ds(start + h * mine, mine), :] = f_ref[:, h * LANES : (h + 1) * LANES]


def forward(plan, table, f_mine, landed, ranges, size):
    return pl.pallas_call(
        functools.partial(forward_kernel, plan, size, ranges),
        out_shape=[
            jax.ShapeDtypeStruct((plan.fwd * size + fock_rows(f_mine), LANES), jnp.float32)
        ]
        * (plan.half - 1),
        in_specs=[pl.BlockSpec(memory_space=pltpu.SMEM)]
        + [pl.BlockSpec(memory_space=pltpu.VMEM)] * (1 + len(landed)),
        out_specs=[pl.BlockSpec(memory_space=pltpu.VMEM)] * (plan.half - 1),
        compiler_params=pltpu.CompilerParams(vmem_limit_bytes=VMEM_LIMIT),
        name="forward",
    )(table, f_mine, *landed)


def split(x):
    high = x.astype(jnp.bfloat16)
    return high, (x - high.astype(jnp.float32)).astype(jnp.bfloat16)


def contract_kernel(plan, tile, parts, pieces, f_piece, table_ref, phase_ref, *refs):
    n = len(pieces)
    ins, out_ref, blocks, dense, f_raw, f_hi, f_lo, sems = refs[:n], *refs[n:]
    step = pl.program_id(0)
    rows = tile * tile
    size = rows * parts
    me = lax.axis_index("row")
    mine, extra = f_piece

    @pl.when(step == 0)
    def _():
        copies = []
        for i, (ref, (start, count, sender)) in enumerate(zip(ins, pieces)):
            got = blocks.at[pl.ds(start * size, count * size)]
            copies.append(pltpu.make_async_copy(ref.at[pl.ds(0, count * size)], got, sems.at[0, i]))
            if sender is not None:
                got = f_raw.at[me ^ sender]
                part = ref.at[pl.ds(count * size, extra)]
                copies.append(pltpu.make_async_copy(part, got, sems.at[1, i]))
        for copy in copies:
            copy.start()
        for copy in copies:
            copy.wait()
        for device in range(plan.nrows):
            for h in range(f_hi.shape[1] // LANES):
                high, low = split(f_raw[device, h * mine : (h + 1) * mine, :])
                at = pl.ds(device * mine, mine), pl.ds(h * LANES, LANES)
                f_hi[at] = high
                f_lo[at] = low

    within = step // tile
    b = step - within * tile
    column = ((me - phase_ref[0]) & (plan.nrows - 1)) + within * plan.nrows
    b_global = column * tile + b
    sub = lax.broadcasted_iota(jnp.int32, (8, LANES), 0)
    for a in range(NT):
        code = table_ref[0, plan.at_loc + within * NT + a]
        for h in range(parts):
            base = code * size + h * rows
            for r in range(0, 16, 8):
                c_global = a * tile + r + sub
                left = blocks[pl.ds(base + b + r * tile, 8, stride=tile), :]
                right = blocks[pl.ds(base + b * tile + r, 8), :]
                value = jnp.where(
                    c_global < b_global, left, jnp.where(c_global > b_global, -right, 0.0)
                )
                if r + 8 > tile:
                    value = jnp.where(sub < tile - r, value, 0.0)
                dense[pl.ds(a * 16 + r, 8), pl.ds(h * LANES, LANES)] = value
    hi, lo = split(dense[...])
    dot = functools.partial(jnp.dot, preferred_element_type=jnp.float32)
    out_ref[0, 0] = dot(f_hi[...], hi) + (dot(f_lo[...], hi) + dot(f_hi[...], lo))


def contract(plan, table, new_phase, buffers, f_piece, tile, occ):
    parts = occ // LANES
    size = tile * tile * parts
    total = plan.n_send + plan.n_fwd
    width = plan.nrows * f_piece[0]
    pieces = tuple(buffer[:3] for buffer in buffers)
    return pl.pallas_call(
        functools.partial(contract_kernel, plan, tile, parts, pieces, f_piece),
        grid=(plan.per * tile,),
        out_shape=jax.ShapeDtypeStruct((plan.per, tile, width, occ), jnp.float32),
        in_specs=[pl.BlockSpec(memory_space=pltpu.SMEM)] * 2
        + [pl.BlockSpec(memory_space=pl.ANY)] * len(buffers),
        out_specs=pl.BlockSpec((1, 1, width, occ), lambda i: (i // tile, i % tile, 0, 0)),
        scratch_shapes=[
            pltpu.VMEM((total * size + 16 * tile, LANES), jnp.float32),
            pltpu.VMEM((NT * 16, occ), jnp.float32),
            pltpu.VMEM((plan.nrows, f_piece[1], LANES), jnp.float32),
            pltpu.VMEM((width, NT * 16), jnp.bfloat16),
            pltpu.VMEM((width, NT * 16), jnp.bfloat16),
            pltpu.SemaphoreType.DMA((2, len(buffers))),
        ],
        compiler_params=pltpu.CompilerParams(
            dimension_semantics=("arbitrary",), vmem_limit_bytes=VMEM_LIMIT
        ),
        name="contract",
    )(table, new_phase, *[buffer[3] for buffer in buffers])


def body(amplitudes, old_blocks, old_counts, new_phase, fock):
    nrows = lax.axis_size("row")
    slots, tile, _, occ = amplitudes.shape
    plan = Plan(nrows, slots)
    half, cap = plan.half, plan.cap
    size = tile * tile * occ // LANES

    def send(x, k):
        return lax.ppermute(x, "row", [(i, i ^ k) for i in range(nrows)])

    table = route(plan, old_blocks, old_counts, new_phase)
    mine = fock.shape[0]
    f_mine = jnp.pad(fock.reshape(mine, NT, tile), ((0, 0), (0, 0), (0, 16 - tile)))
    f_mine = f_mine.reshape(mine, NT * 16)
    f_piece = mine, fock_rows(f_mine)
    amp = jnp.transpose(amplitudes, (1, 2, 0, 3)).reshape(tile * tile, slots, occ)

    def branch(wide, soon, following, table, amp, new_phase, f_mine):
        late = wide - soon
        side, next_to, far = range(1, plan.quarter), range(plan.quarter, half), range(half, nrows)
        head = [(k * cap, following, False) for k in next_to]
        head += [(k * cap, soon, not late) for k in far]
        head = dict(zip([*next_to, *far], pack(table, amp, f_mine, head)))
        landed = {k: send(head[k], k) for k in next_to}
        landed |= {k: send(head[k], k) for k in far}
        rest = [(k * cap, cap, k == 0) for k in (0, *side)]
        rest += [(k * cap + soon, late, True) for k in far if late]
        rest = pack(table, amp, f_mine, rest)
        side_in = {k: send(rest[k], k) for k in side}
        late_in = {k: send(rest[k - nrows], k) for k in far if late}
        ranges = [(k * cap, soon if k >= half else following) for k in landed]
        relay = forward(plan, table, f_mine, list(landed.values()), ranges, size)
        relay_in = {k: send(relay[k - 1], k) for k in range(1, half)}
        buffers = [(0, cap, 0, rest[0])]
        buffers += [(k * cap, cap, None, side_in[k]) for k in side]
        buffers += [(k * cap, following, None, landed[k]) for k in next_to]
        buffers += [(k * cap, soon, None if late else k, landed[k]) for k in far]
        buffers += [(k * cap + soon, late, k, late_in[k]) for k in late_in]
        buffers += [(plan.at_fwd + (k - 1) * plan.fwd, plan.fwd, k, relay_in[k]) for k in relay_in]
        return contract(plan, table, new_phase, buffers, f_piece, tile, occ)

    return lax.switch(
        table[0, plan.at_level],
        [functools.partial(branch, *level) for level in plan.levels],
        table,
        amp,
        new_phase,
        f_mine,
    )


def solution(mesh):
    return jax.shard_map(
        body,
        mesh=mesh,
        in_specs=(P("row", None, None, "col"), P(), P(), P(), P("row", None)),
        out_specs=P("row", None, None, "col"),
        check_vma=False,
    )
```

```python
import functools

import jax
import jax.numpy as jnp
from jax import lax
from jax.experimental import pallas as pl
from jax.experimental.pallas import tpu as pltpu
from jax.sharding import PartitionSpec as P


NT = 16
LANES = 128
VMEM_LIMIT = 67_000_000


class Plan:
    def __init__(self, nrows, slots):
        self.nrows = nrows
        self.half = nrows // 2
        self.quarter = nrows // 4
        self.per = NT // nrows
        self.cap = self.per * ((slots - 2) // 8 + 2)
        self.fwd = self.per * self.per
        self.n_send = nrows * self.cap
        self.n_fwd = (self.half - 1) * self.fwd
        self.n_loc = self.per * NT
        self.at_fwd = self.n_send
        self.at_loc = self.n_send + self.n_fwd
        self.at_level = self.at_loc + self.n_loc
        cap = self.cap
        part = [-(-i * cap // 8) for i in range(9)]
        levels = (
            (part[5], part[3], part[6]),
            (part[5], part[4], cap),
            (part[6], part[3], part[6]),
            (part[6], part[5], cap),
            (cap, cap, cap),
        )
        self.levels = tuple(dict.fromkeys(levels))


def route_kernel(plan, slots, ids_ref, counts_ref, phase_ref, out_ref):
    nrows, half, per, cap = plan.nrows, plan.half, plan.per, plan.cap
    me = lax.axis_index("row")
    phase = phase_ref[0]
    ids = jnp.transpose(ids_ref[...].astype(jnp.float32)).astype(jnp.int32)
    first = jnp.zeros_like(ids)
    for t in range(1, NT):
        first = first + (ids >= t * NT - t * (t - 1) // 2).astype(jnp.int32)
    second = ids - (first * NT - lax.shift_right_logical(first * (first - 1), 1)) + first
    src = lax.broadcasted_iota(jnp.int32, ids.shape, 1)
    slot = lax.broadcasted_iota(jnp.int32, ids.shape, 0)
    live = slot < counts_ref[...]
    low = (first + phase) & (nrows - 1)
    high = (second + phase) & (nrows - 1)
    shift = nrows.bit_length() - 1
    w_low = lax.shift_right_logical(first, shift)
    w_high = lax.shift_right_logical(second, shift)
    pair_part = jnp.where(low < high, w_low * per + w_high, w_high * per + w_low)
    same = low == high
    one = jnp.int32(1)
    zero = jnp.int32(0)

    def flag(x):
        return jnp.where(x, one, zero)

    def group(owner):
        away = owner ^ src
        return jnp.where((away & half) != 0, 2, flag((away & plan.quarter) != 0))

    g_low, g_high = group(low), group(high)
    shared = flag(live & (g_low == g_high) & (g_low > 0) & ~same)
    on_low = flag(live) * (1 - shared)
    on_high = flag(live & ~same) * (1 - shared)
    dest = lax.broadcasted_iota(jnp.int32, (nrows, nrows), 0)
    away = dest ^ lax.broadcasted_iota(jnp.int32, (nrows, nrows), 1)
    is_far = (away & half) != 0
    is_next = ~is_far & ((away & plan.quarter) != 0)

    def row(x, s):
        return x[s : s + 1, :]

    def hit(x, on, s):
        return jnp.where((dest == row(x, s)) & (row(on, s) == 1), 1.0, 0.0)

    def at(mask, run):
        return jnp.sum(mask * run, axis=0, keepdims=True)

    count = jnp.zeros((nrows, nrows), jnp.float32)
    for s in range(slots):
        count = count + hit(low, on_low, s) + hit(high, on_high, s)
    early = jnp.zeros((nrows, nrows), jnp.float32)
    land_rows, pos_rows, low_rows, high_rows = [], [], [], []
    for s in range(slots):
        m_low = hit(low, shared, s)
        m_high = hit(high, shared, s)
        take = at(m_low, count) <= at(m_high, count)
        mask = jnp.where(take, m_low, m_high)
        pos_rows.append(at(mask, early))
        land_rows.append(jnp.where(take, row(low, s), row(high, s)))
        early = early + mask
        count = count + mask
    run = early
    for s in range(slots):
        m_low, m_high = hit(low, on_low, s), hit(high, on_high, s)
        low_rows.append(at(m_low, run))
        high_rows.append(at(m_high, run))
        run = run + m_low + m_high

    def top(x):
        return jnp.max(jnp.max(x, axis=0, keepdims=True), axis=1, keepdims=True)

    most = top(jnp.where(is_far, count, 0.0))
    most_early = top(jnp.where(is_far, early, 0.0))
    most_next = top(jnp.where(is_next, count, 0.0))
    level = jnp.full((1, 1), float(len(plan.levels) - 1), jnp.float32)
    for i in range(len(plan.levels) - 2, -1, -1):
        wide, soon, following = plan.levels[i]
        fits = (most <= wide) & (most_early <= soon) & (most_next <= following)
        level = jnp.where(fits, float(i), level)

    lane = lax.broadcasted_iota(jnp.int32, (1, nrows), 1)
    e_send = lax.broadcasted_iota(jnp.int32, (plan.n_send, nrows), 0)
    e_fwd = lax.broadcasted_iota(jnp.int32, (plan.n_fwd, nrows), 0)
    e_loc = lax.broadcasted_iota(jnp.int32, (plan.n_loc, nrows), 0)
    t_send = jnp.zeros((plan.n_send, nrows), jnp.int32)
    t_fwd = jnp.zeros((plan.n_fwd, nrows), jnp.int32)
    t_loc = jnp.zeros((plan.n_loc, nrows), jnp.int32)
    mine = lane == me

    def put(table, index, where_, value, on):
        return table + jnp.where(index == jnp.where(on, where_, -1), value, 0)

    for s in range(slots):
        lo, hi, land = row(low, s), row(high, s), land_rows[s]
        both = row(shared, s) == 1
        p_low = low_rows[s].astype(jnp.int32)
        p_high = high_rows[s].astype(jnp.int32)
        other = lo + hi - land
        k_low = (lo ^ lane) * cap + p_low
        k_high = (hi ^ lane) * cap + p_high
        k_land = (land ^ lane) * cap + pos_rows[s].astype(jnp.int32)
        value = jnp.full((1, nrows), s, jnp.int32)
        t_send = put(t_send, e_send, k_low, value, (row(on_low, s) == 1) & mine)
        t_send = put(t_send, e_send, k_high, value, (row(on_high, s) == 1) & mine)
        t_send = put(t_send, e_send, k_land, value, both & mine)
        part = row(pair_part, s)
        t_fwd = put(t_fwd, e_fwd, ((land ^ other) - 1) * plan.fwd + part, k_land, both & (land == me))
        lo_me, hi_me = lo == me, hi == me
        k_both = jnp.where(land == me, k_land, plan.at_fwd + ((land ^ me) - 1) * plan.fwd + part)
        code = jnp.where(both, k_both, jnp.where(lo_me, k_low, k_high))
        a, b = row(first, s), row(second, s)
        ok = row(flag(live), s) == 1
        t_loc = put(t_loc, e_loc, row(w_low, s) * NT + b, code, ok & lo_me)
        t_loc = put(t_loc, e_loc, row(w_high, s) * NT + a, code, ok & hi_me & (a != b))

    def column(table):
        return jnp.sum(table.astype(jnp.float32), axis=1, keepdims=True)

    wide_lane = out_ref.shape[1]

    def spread(table, start):
        col = column(table)
        shape = (col.shape[0], wide_lane)
        down = lax.broadcasted_iota(jnp.int32, shape, 0) + start
        across = lax.broadcasted_iota(jnp.int32, shape, 1)
        return jnp.sum(jnp.where(down == across, col, 0.0), axis=0, keepdims=True)

    line = spread(t_send, 0) + spread(t_fwd, plan.at_fwd) + spread(t_loc, plan.at_loc)
    across = lax.broadcasted_iota(jnp.int32, (1, wide_lane), 1)
    line = jnp.where(across == plan.at_level, level, line)
    out_ref[...] = line.astype(jnp.int32)


def route(plan, old_blocks, old_counts, new_phase):
    nrows, slots = old_blocks.shape
    wide = -(-(plan.at_level + 1) // LANES) * LANES
    return pl.pallas_call(
        functools.partial(route_kernel, plan, slots),
        out_shape=jax.ShapeDtypeStruct((1, wide), jnp.int32),
        in_specs=[
            pl.BlockSpec(memory_space=pltpu.VMEM),
            pl.BlockSpec(memory_space=pltpu.VMEM),
            pl.BlockSpec(memory_space=pltpu.SMEM),
        ],
        out_specs=pl.BlockSpec(memory_space=pltpu.VMEM),
        name="route",
    )(old_blocks, old_counts.reshape(1, nrows), new_phase)


def pack_kernel(streams, slots_pad, parts, table_ref, *refs):
    rows = refs[0].shape[0]
    flats = [ref.reshape(rows * slots_pad, LANES) for ref in refs[:parts]]
    f_refs, outs = refs[parts:-len(streams)], refs[-len(streams) :]
    for (base, count, carries), out in zip(streams, outs):

        def one(j, carry, base=base, out=out):
            slot = table_ref[0, base + j]
            for h, flat in enumerate(flats):
                for r in range(0, rows, 8):
                    n = min(8, rows - r)
                    piece = flat[pl.ds(r * slots_pad + slot, n, stride=slots_pad), :]
                    out[pl.ds(j * rows * parts + h * rows + r, n), :] = piece
            return carry

        lax.fori_loop(0, count, one, 0)
        if carries:
            write_fock(f_refs[0], out, count * rows * parts)


def fock_rows(f_mine):
    return -(-f_mine.shape[0] * -(-f_mine.shape[1] // LANES) // 8) * 8


def pack(table, amp, f_mine, streams):
    rows, slots, occ = amp.shape
    parts = occ // LANES
    pad = -(-slots // 8) * 8
    pad += 8 * (pad // 8 % 2 == 0)
    extra = fock_rows(f_mine)
    shapes = [(n * rows * parts + (extra if c else 0), LANES) for _, n, c in streams]
    f_args = [f_mine] if any(c for _, _, c in streams) else []
    return pl.pallas_call(
        functools.partial(pack_kernel, streams, pad, parts),
        out_shape=[jax.ShapeDtypeStruct(shape, jnp.float32) for shape in shapes],
        in_specs=[
            pl.BlockSpec(memory_space=pltpu.SMEM),
            *[pl.BlockSpec((rows, pad, LANES), lambda i, h=h: (0, 0, h)) for h in range(parts)],
            *[pl.BlockSpec(x.shape, lambda i: (0, 0)) for x in f_args],
        ],
        out_specs=[pl.BlockSpec(shape, lambda i: (0, 0)) for shape in shapes],
        grid=(1,),
        compiler_params=pltpu.CompilerParams(vmem_limit_bytes=VMEM_LIMIT),
        name="pack",
    )(table, *[amp] * parts, *f_args)


def forward_kernel(plan, size, ranges, f_piece, table_ref, f_ref, *refs):
    ins, outs = refs[: len(ranges)], refs[len(ranges) :]
    extra, partner, f_at = f_piece
    for k, out in enumerate(outs):

        def one(j, carry, k=k, out=out):
            code = table_ref[0, plan.at_fwd + k * plan.fwd + j]
            for ref, (start, count) in zip(ins, ranges):

                @pl.when((code >= start) & (code < start + count))
                def _(ref=ref, start=start):
                    to, of = pl.multiple_of(j * size, 8), pl.multiple_of((code - start) * size, 8)
                    out[pl.ds(to, size), :] = ref[pl.ds(of, size), :]

            return carry

        lax.fori_loop(0, plan.fwd, one, 0)
        write_fock(f_ref, out, plan.fwd * size)
        out[pl.ds(plan.fwd * size + extra, extra), :] = ins[partner][pl.ds(f_at, extra), :]


def write_fock(f_ref, out, start):
    mine, wide = f_ref.shape
    for h in range(-(-wide // LANES)):
        piece = f_ref[:, h * LANES : min(wide, (h + 1) * LANES)]
        if piece.shape[1] < LANES:
            blank = jnp.zeros((mine, LANES - piece.shape[1]), jnp.float32)
            piece = jnp.concatenate([piece, blank], axis=1)
        out[pl.ds(start + h * mine, mine), :] = piece


def forward(plan, table, f_mine, landed, ranges, size):
    extra = fock_rows(f_mine)
    partner = [start for start, _ in ranges].index(plan.half * plan.cap)
    f_piece = extra, partner, ranges[partner][1] * size
    return pl.pallas_call(
        functools.partial(forward_kernel, plan, size, ranges, f_piece),
        out_shape=[
            jax.ShapeDtypeStruct((plan.fwd * size + 2 * extra, LANES), jnp.float32)
        ]
        * (plan.half - 1),
        in_specs=[pl.BlockSpec(memory_space=pltpu.SMEM)]
        + [pl.BlockSpec(memory_space=pltpu.VMEM)] * (1 + len(landed)),
        out_specs=[pl.BlockSpec(memory_space=pltpu.VMEM)] * (plan.half - 1),
        compiler_params=pltpu.CompilerParams(vmem_limit_bytes=VMEM_LIMIT),
        name="forward",
    )(table, f_mine, *landed)


def split(x):
    high = x.astype(jnp.bfloat16)
    return high, (x - high.astype(jnp.float32)).astype(jnp.bfloat16)


def contract_kernel(plan, tile, parts, group, pieces, f_piece, table_ref, phase_ref, *refs):
    n = len(pieces)
    ins, out_ref, blocks = refs[:n], refs[n], refs[n + 1]
    dense, (f_raw, f_full, f_hi, f_lo, sems) = refs[n + 2 : n + 2 + group], refs[n + 2 + group :]
    rows = tile * tile
    size = rows * parts
    me = lax.axis_index("row")
    mine, extra = f_piece
    dot = functools.partial(jnp.dot, preferred_element_type=jnp.float32)

    @pl.when(pl.program_id(0) == 0)
    def _():
        copies = []
        for i, (ref, (start, count, senders)) in enumerate(zip(ins, pieces)):
            got = blocks.at[pl.ds(start * size, count * size)]
            copies.append(pltpu.make_async_copy(ref.at[pl.ds(0, count * size)], got, sems.at[0, i]))
            for j, sender in enumerate(senders):
                got = f_raw.at[me ^ sender]
                part = ref.at[pl.ds(count * size + j * extra, extra)]
                copies.append(pltpu.make_async_copy(part, got, sems.at[1 + j, i]))
        for copy in copies:
            copy.start()
        for copy in copies:
            copy.wait()
        f_full[...] = jnp.zeros_like(f_full)
        width = plan.nrows * mine
        for device in range(plan.nrows):
            for h in range(-(-width // LANES)):
                piece = f_raw[device, h * mine : (h + 1) * mine, :]
                f_full[pl.ds(device * mine, mine), pl.ds(h * LANES, LANES)] = piece
        shape = (f_full.shape[1], f_hi.shape[1])
        old = lax.broadcasted_iota(jnp.int32, shape, 0)
        new = lax.broadcasted_iota(jnp.int32, shape, 1)
        moved = (lax.shift_right_logical(new, 4) * tile + (new & 15) == old) & ((new & 15) < tile)
        move = jnp.where(moved, 1.0, 0.0).astype(jnp.bfloat16)
        high, low = split(f_full[...])
        f_hi[...] = dot(high, move).astype(jnp.bfloat16)
        f_lo[...] = dot(low, move).astype(jnp.bfloat16)

    sub = lax.broadcasted_iota(jnp.int32, (8, LANES), 0)
    for g in range(group):
        step = pl.program_id(0) * group + g
        within = step // tile
        b = step - within * tile
        column = ((me - phase_ref[0]) & (plan.nrows - 1)) + within * plan.nrows
        b_global = column * tile + b
        for a in range(NT):
            code = table_ref[0, plan.at_loc + within * NT + a]
            for h in range(parts):
                base = code * size + h * rows
                for r in range(0, 16, 8):
                    c_global = a * tile + r + sub
                    left = blocks[pl.ds(base + b + r * tile, 8, stride=tile), :]
                    right = blocks[pl.ds(base + b * tile + r, 8), :]
                    value = jnp.where(
                        c_global < b_global, left, jnp.where(c_global > b_global, -right, 0.0)
                    )
                    if r + 8 > tile:
                        value = jnp.where(sub < tile - r, value, 0.0)
                    dense[g][pl.ds(a * 16 + r, 8), pl.ds(h * LANES, LANES)] = value
    for g in range(group):
        hi, lo = split(dense[g][...])
        out_ref[0, g] = dot(f_hi[...], hi) + (dot(f_lo[...], hi) + dot(f_hi[...], lo))


def contract(plan, table, new_phase, buffers, f_piece, tile, occ):
    parts = occ // LANES
    size = tile * tile * parts
    total = plan.n_send + plan.n_fwd
    width = plan.nrows * f_piece[0]
    pieces = tuple(buffer[:3] for buffer in buffers)
    group = 2 if tile % 2 == 0 else 1
    per = tile // group
    wide = -(-width // LANES) * LANES
    return pl.pallas_call(
        functools.partial(contract_kernel, plan, tile, parts, group, pieces, f_piece),
        grid=(plan.per * per,),
        out_shape=jax.ShapeDtypeStruct((plan.per, tile, width, occ), jnp.float32),
        in_specs=[pl.BlockSpec(memory_space=pltpu.SMEM)] * 2
        + [pl.BlockSpec(memory_space=pl.ANY)] * len(buffers),
        out_specs=pl.BlockSpec((1, group, width, occ), lambda i: (i // per, i % per, 0, 0)),
        scratch_shapes=[
            pltpu.VMEM((total * size + 16 * tile, LANES), jnp.float32),
            *[pltpu.VMEM((NT * 16, occ), jnp.float32)] * group,
            pltpu.VMEM((plan.nrows, f_piece[1], LANES), jnp.float32),
            pltpu.VMEM((width, wide), jnp.float32),
            pltpu.VMEM((width, NT * 16), jnp.bfloat16),
            pltpu.VMEM((width, NT * 16), jnp.bfloat16),
            pltpu.SemaphoreType.DMA((3, len(buffers))),
        ],
        compiler_params=pltpu.CompilerParams(
            dimension_semantics=("arbitrary",), vmem_limit_bytes=VMEM_LIMIT
        ),
        name="contract",
    )(table, new_phase, *[buffer[3] for buffer in buffers])


def body(amplitudes, old_blocks, old_counts, new_phase, fock):
    nrows = lax.axis_size("row")
    slots, tile, _, occ = amplitudes.shape
    plan = Plan(nrows, slots)
    half, cap = plan.half, plan.cap
    size = tile * tile * occ // LANES

    def send(x, k):
        return lax.ppermute(x, "row", [(i, i ^ k) for i in range(nrows)])

    table = route(plan, old_blocks, old_counts, new_phase)
    mine = fock.shape[0]
    f_piece = mine, fock_rows(fock)
    amp = jnp.transpose(amplitudes, (1, 2, 0, 3)).reshape(tile * tile, slots, occ)

    def branch(wide, soon, following, table, amp, new_phase, f_mine):
        late = wide - soon
        side, next_to, far = range(1, plan.quarter), range(plan.quarter, half), range(half, nrows)
        head = [(half * cap, soon, True)]
        head += [(k * cap, following, False) for k in next_to]
        head += [(k * cap, soon, False) for k in far[1:]]
        head = dict(zip([half, *next_to, *far[1:]], pack(table, amp, f_mine, head)))
        landed = {half: send(head[half], half)}
        landed |= {k: send(head[k], k) for k in next_to}
        landed |= {k: send(head[k], k) for k in far[1:]}
        rest = [(k * cap, cap, k == 0) for k in (0, *side)]
        rest += [(k * cap + soon, late, False) for k in far if late]
        rest = pack(table, amp, f_mine, rest)
        side_in = {k: send(rest[k], k) for k in side}
        late_in = {}
        for k in far if late else ():
            late_in[k] = send(rest[k - nrows], k)
        ranges = [(k * cap, soon if k >= half else following) for k in landed]
        relay = forward(plan, table, f_mine, list(landed.values()), ranges, size)
        relay_in = {k: send(relay[k - 1], k) for k in range(1, half)}
        buffers = [(0, cap, (0,), rest[0])]
        buffers += [(k * cap, cap, (), side_in[k]) for k in side]
        buffers += [(k * cap, following, (), landed[k]) for k in next_to]
        buffers += [(k * cap, soon, (k,) if k == half else (), landed[k]) for k in far]
        buffers += [(k * cap + soon, late, (), late_in[k]) for k in late_in]
        for k in relay_in:
            start = plan.at_fwd + (k - 1) * plan.fwd
            buffers.append((start, plan.fwd, (k, k ^ half), relay_in[k]))
        return contract(plan, table, new_phase, buffers, f_piece, tile, occ)

    return lax.switch(
        table[0, plan.at_level],
        [functools.partial(branch, *level) for level in plan.levels],
        table,
        amp,
        new_phase,
        fock,
    )


def solution(mesh):
    return jax.shard_map(
        body,
        mesh=mesh,
        in_specs=(P("row", None, None, "col"), P(), P(), P(), P("row", None)),
        out_specs=P("row", None, None, "col"),
        check_vma=False,
    )
```
